32 devices in a mesh: gx: 2 (over x), gy: 8 (over z, y), lev: 2 (over core).
Axes of the slice: x: 2, y: 2, z: 4, core: 2. Of those that a mesh axis runs over, the one named last changes fastest.
Arguments:
- fine_state: float32 [3, 32, 192, 768], P(None, 'lev', 'gy', 'gx'), may hold values from -6 to 6
- wind_field: float32 [2, 32, 192, 768], P(None, 'lev', 'gy', 'gx'), may hold values from -4 to 4
- increment: float32 [3, 32, 48, 192], P(None, 'lev', 'gy', 'gx'), may hold values from -6 to 6
- misfit: float32 [3, 32, 48, 192], P(None, 'lev', 'gy', 'gx'), may hold values from -6 to 6
Outputs:
- fine_next: float32 [3, 32, 192, 768], P(None, 'lev', 'gy', 'gx')
- gradient: float32 [3, 32, 48, 192], P(None, 'lev', 'gy', 'gx')
The draws below stay inside these ranges and needn't reach their ends.
All inputs are finite; a program needn't handle non-finite values.
Results may differ from the reference program's by a relative error of at most 0.000078.
Values sent between devices are 32-bit elements; how exact they have to be, the bound alone decides.
No kernel may reach another device: no remote copies, remote signals or barrier semaphores. Data moves between devices by JAX's collectives and lax.ppermute only.
A program may use at most 64 MiB of HBM per device.

```python
import jax
import jax.numpy as jnp
from jax import lax

VARS = 3
LEVELS = 32
NY = 192
NX = 768
CNY = 48
CNX = 192


def block_scale(key, shape, split, smallest, largest):
    gain = 1.0
    for position, parts in split:
        steps = jax.random.uniform(jax.random.fold_in(jax.random.fold_in(key, 6), position), (parts,), jnp.float32, smallest / len(split), largest / len(split))
        gain = gain * jnp.repeat(jnp.exp(steps), shape[position] // parts).reshape((-1,) + (1,) * (len(shape) - 1 - position))
    return gain


def scatter_about(rng, extent, scale, limit, split=(), dtype=jnp.bfloat16):
    drawn = jax.random.normal(rng, extent, jnp.float32) * scale
    if len(split) > 0:
        drawn = block_scale(rng, extent, split, -0.22, 0.18) * drawn
    return jnp.clip(drawn, min=-limit, max=limit).astype(dtype)


def setup_inputs(seed: int = 0) -> dict:
    streams_of = jax.random.split(jax.random.key(seed), 5)
    return {
        "fine_state": scatter_about(streams_of[0], (VARS, LEVELS, NY, NX), 1.0, 6.0, ((1, 2), (2, 8), (3, 2)), jnp.float32),
        "wind_field": scatter_about(streams_of[1], (2, LEVELS, NY, NX), 1.0, 4.0, ((1, 2), (2, 8), (3, 2)), jnp.float32),
        "increment": scatter_about(streams_of[2], (VARS, LEVELS, CNY, CNX), 1.0, 6.0, ((1, 2), (2, 8), (3, 2)), jnp.float32),
        "misfit": scatter_about(streams_of[3], (VARS, LEVELS, CNY, CNX), 1.0, 6.0, ((1, 2), (2, 8), (3, 2)), jnp.float32),
    }


advect = 0.25
vertical_mix = 0.1
damping = 0.3
descent = 0.5


def mixing():
    return jnp.array([0.05, 0.1, 0.2], jnp.float32).reshape(3, 1, 1, 1)


def pad_all(values):
    leading = [(0, 0)] * (values.ndim - 3)
    padded = jnp.pad(values, leading + [(1, 1), (1, 1), (0, 0)])
    return jnp.concatenate([padded[..., -1:], padded, padded[..., :1]], axis=-1)


def laplace_terms(padded):
    center = padded[:, 1:-1, 1:-1, 1:-1]
    planar = padded[:, 1:-1, 1:-1, 2:] + padded[:, 1:-1, 1:-1, :-2] + padded[:, 1:-1, 2:, 1:-1] + padded[:, 1:-1, :-2, 1:-1] - 4.0 * center
    column = padded[:, 2:, 1:-1, 1:-1] + padded[:, :-2, 1:-1, 1:-1] - 2.0 * center
    return center, mixing() * planar + vertical_mix * column


def forward_linear(padded, wind_center):
    center, spread = laplace_terms(padded)
    along_x = 0.5 * (padded[:, 1:-1, 1:-1, 2:] - padded[:, 1:-1, 1:-1, :-2])
    along_y = 0.5 * (padded[:, 1:-1, 2:, 1:-1] - padded[:, 1:-1, :-2, 1:-1])
    return center - advect * (wind_center[0] * along_x + wind_center[1] * along_y) + spread


def adjoint_linear(padded, wind_pad):
    center, spread = laplace_terms(padded)
    flux_x = wind_pad[0] * padded
    flux_y = wind_pad[1] * padded
    along_x = 0.5 * (flux_x[:, 1:-1, 1:-1, 2:] - flux_x[:, 1:-1, 1:-1, :-2])
    along_y = 0.5 * (flux_y[:, 1:-1, 2:, 1:-1] - flux_y[:, 1:-1, :-2, 1:-1])
    return center + advect * (along_x + along_y) + spread


def slope(state):
    squashed = jnp.tanh(state)
    return damping * (1.0 - squashed * squashed)


def restrict(values):
    dims_now = values.shape
    blocks = values.reshape(dims_now[0], dims_now[1], dims_now[2] // 4, 4, dims_now[3] // 4, 4)
    return jnp.mean(blocks, axis=(3, 5))


def coarse_chain(extend, cstate, cwinds, increment, misfit):
    variables = cstate.shape[0]
    stacked = extend(jnp.concatenate([cwinds, cstate, increment], axis=0))
    wind_pad = stacked[:2]
    trajectory = forward_linear(stacked[2:2 + variables], cwinds) - damping * jnp.tanh(cstate)
    delta_one = forward_linear(stacked[2 + variables:], cwinds) - slope(cstate) * increment
    delta_two = forward_linear(extend(delta_one), cwinds) - slope(trajectory) * delta_one
    residual = delta_two - misfit
    adjoint_one = adjoint_linear(extend(residual), wind_pad) - slope(trajectory) * residual
    adjoint_zero = adjoint_linear(extend(adjoint_one), wind_pad) - slope(cstate) * adjoint_one
    gradient = increment + adjoint_zero
    return gradient, increment - descent * gradient


def prolong(padded, axis):
    number = padded.shape[axis] - 2
    left = lax.slice_in_dim(padded, 0, number, axis=axis)
    middle = lax.slice_in_dim(padded, 1, number + 1, axis=axis)
    right = lax.slice_in_dim(padded, 2, number + 2, axis=axis)
    pieces = [0.375 * left + 0.625 * middle, 0.125 * left + 0.875 * middle,
              0.875 * middle + 0.125 * right, 0.625 * middle + 0.375 * right]
    joined = jnp.stack(pieces, axis=axis + 1)
    target = list(padded.shape)
    target[axis] = 4 * number
    return joined.reshape(target)


def reference(fine_state, wind_field, increment, misfit):
    cstate = restrict(fine_state)
    cwinds = restrict(wind_field)
    gradient, updated = coarse_chain(pad_all, cstate, cwinds, increment, misfit)
    widened = pad_all(updated)[:, 1:-1]
    fine_increment = prolong(prolong(widened, 3), 2)
    fine_new = fine_state + fine_increment
    fine_next = forward_linear(pad_all(fine_new), wind_field) - damping * jnp.tanh(fine_new)
    return fine_next, gradient
```

```python
import functools

import jax
import jax.numpy as jnp
from jax import lax
from jax.experimental import pallas as pl
from jax.experimental.pallas import tpu as pltpu
from jax.sharding import PartitionSpec as P

advect = 0.25
vertical_mix = 0.1
damping = 0.3
descent = 0.5
mixing = (0.05, 0.1, 0.2)
ratio = 4
LANES = 128
TILE = 8
H_INC, H_ST, H_MIS = 5, 4, 3
f32 = jnp.float32
bf16 = jnp.bfloat16


def roll(x, shift, axis):
    size = x.shape[axis]
    shift = shift % size
    return x if shift == 0 else pltpu.roll(x, shift, axis)


def lane_of(shape):
    return lax.broadcasted_iota(jnp.int32, shape, len(shape) - 1)


def split3(x):
    hi = x.astype(bf16)
    rest = x - hi.astype(f32)
    mid = rest.astype(bf16)
    low = (rest - mid.astype(f32)).astype(bf16)
    return hi, mid, low


def exact_dot(x, table):
    hi, mid, low = split3(x)
    dot = functools.partial(jnp.dot, preferred_element_type=f32)
    return dot(hi, table) + (dot(mid, table) + dot(low, table))


def pack_quad(rows, cols):
    r0, r1, r2, r3 = rows
    lane = lane_of(r0.shape)
    t1 = roll(r1, cols, 1)
    t2 = roll(r2, 2 * cols - LANES, 1)
    t3 = roll(r3, 3 * cols - 2 * LANES, 1)
    return (
        jnp.where(lane < cols, r0, t1),
        jnp.where(lane < 2 * cols - LANES, t1, t2),
        jnp.where(lane < 3 * cols - 2 * LANES, t2, t3),
    )


def unpack_quad(packed, index, cols):
    p0, p1, p2 = packed
    if index == 0:
        return p0
    lane = lane_of(p0.shape)
    if index == 1:
        edge = LANES - cols
        return jnp.where(lane < edge, roll(p0, edge, 1), roll(p1, edge, 1))
    if index == 2:
        edge = 2 * (LANES - cols)
        return jnp.where(lane < edge, roll(p1, edge, 1), roll(p2, edge, 1))
    return roll(p2, 3 * (LANES - cols), 1)


def edge_lanes(x, cols, h):
    lane = lane_of(x.shape)
    return jnp.where(lane < h, x, roll(x, LANES - cols, 1))


def put_slot(acc, x, slot, h, cols):
    lane = lane_of(x.shape)
    moved = roll(edge_lanes(x, cols, h), 2 * h * slot + h, 1)
    inside = jnp.logical_and(lane >= 2 * h * slot, lane < 2 * h * (slot + 1))
    return jnp.where(inside, moved, acc)


def join_columns(own, from_left, from_right, slot, h, cols):
    lane = lane_of(own.shape)
    back = -(2 * h * slot + h)
    left = roll(from_left, back, 1)
    right = roll(from_right, back + cols, 1)
    return jnp.where(lane < cols, own, jnp.where(lane < (cols + LANES) // 2, right, left))


def slots_of(h):
    return LANES // (2 * h)


def ceil_div(a, b):
    return -(-a // b)


def early_slabs(rows):
    inc = [("inc", v, r) for v in range(3) for r in range(-H_INC, rows + H_INC)]
    mis = [("mis", v, r) for v in range(3) for r in range(-H_MIS, rows + H_MIS)]
    return inc, mis


def late_slabs(rows, count):
    return [("st", v, r) for v in range(count) for r in range(-H_ST, rows + H_ST)]


class Early:
    def __init__(self, inc, mis, top, bottom, rows, cols, first, last):
        self.inc, self.mis, self.top, self.bottom = inc, mis, top, bottom
        self.rows, self.cols, self.first, self.last = rows, cols, first, last

    def slab(self, kind, v, r, lev):
        own = self.inc if kind == "inc" else self.mis
        h = H_INC if kind == "inc" else H_MIS
        if 0 <= r < self.rows:
            return own[v, r, lev, :]
        if r < 0:
            ref, place, off = self.top, r + h, self.first
        else:
            ref, place, off = self.bottom, r - self.rows, self.last
        if kind == "mis":
            place += H_INC
        quad, index = divmod(place, 4)
        packed = tuple(ref[v, quad, i, lev, :] for i in range(3))
        value = unpack_quad(packed, index, self.cols)
        return jnp.where(off, jnp.zeros_like(value), value)


class Late:
    def __init__(self, own, top, bottom, rows, cols, first, last):
        self.own, self.top, self.bottom = own, top, bottom
        self.rows, self.cols, self.first, self.last = rows, cols, first, last

    def slab(self, kind, v, r, lev):
        if 0 <= r < self.rows:
            return self.own[v, r, lev, :]
        if r < 0:
            ref, index, off = self.top, r + H_ST, self.first
        else:
            ref, index, off = self.bottom, r - self.rows, self.last
        packed = tuple(ref[v, i, lev, :] for i in range(3))
        value = unpack_quad(packed, index, self.cols)
        return jnp.where(off, jnp.zeros_like(value), value)


def ends(axis):
    place = lax.axis_index(axis)
    return place == 0, place == lax.axis_size(axis) - 1


def fetch(state, wind, held, sems):
    copies = []
    for v in range(5):
        source = wind.at[v] if v < 2 else state.at[v - 2]
        copies.append([])
        for t in range(held.shape[1]):
            part = source.at[:, pl.ds(LANES * t, LANES)]
            copies[-1].append(pltpu.make_async_copy(part, held.at[v, t], sems.at[v, t]))
            copies[-1][-1].start()
    return copies


def wait_all(copies):
    for c in copies:
        c.wait()


def pack_early_kernel(inc, mis, up, down, *, rows, cols):
    for v in range(3):
        first = [inc[v, r] for r in range(H_INC)] + [mis[v, r] for r in range(H_MIS)]
        last = [inc[v, rows - H_INC + r] for r in range(H_INC)]
        last += [mis[v, rows - H_MIS + r] for r in range(H_MIS)]
        for out, seq in ((up, first), (down, last)):
            for quad in range(2):
                for i, value in enumerate(pack_quad(seq[4 * quad : 4 * quad + 4], cols)):
                    out[v, quad, i] = value


def mean_kernel(
    state, wind, coarse, up, down, edge_up, edge_down, edge_x, edge_low, edge_high,
    held, sums, sems, *, levels, rows, cols,
):
    fine_rows = ratio * rows
    fine_cols = ratio * cols
    copies = fetch(state, wind, held, sems)
    source_col = lax.broadcasted_iota(jnp.int32, (fine_cols, LANES), 0)
    target_col = lax.broadcasted_iota(jnp.int32, (fine_cols, LANES), 1)
    table = jnp.where(source_col // ratio == target_col, 1.0 / (ratio * ratio), 0.0).astype(bf16)
    slot_h = 2
    per = slots_of(slot_h)
    acc = None
    for v in range(5):
        wait_all(copies[v])
        for row in range(rows):
            total = None
            for a in range(ratio):
                f = ratio * row + a
                pieces = [
                    held[v, t, pl.ds(f, levels, stride=fine_rows), :]
                    for t in range(fine_cols // LANES)
                ]
                slab = jnp.concatenate(pieces, axis=1)
                total = slab if total is None else total + slab
                if v >= 2:
                    if f == 0:
                        edge_up[v - 2] = slab
                    if f == fine_rows - 1:
                        edge_down[v - 2] = slab
                    index = (v - 2) * fine_rows + f
                    group, slot = divmod(index, per)
                    lane = lane_of(pieces[0].shape)
                    seam = jnp.where(lane < LANES // 2, pieces[0], pieces[-1])
                    moved = roll(seam, 2 * slot_h * slot + slot_h, 1)
                    if slot == 0:
                        acc = moved
                    else:
                        acc = jnp.where(lane >= 2 * slot_h * slot, moved, acc)
                    if slot == per - 1 or index == 3 * fine_rows - 1:
                        edge_x[group] = acc
            sums[pl.ds((v * rows + row) * levels, levels), :] = total
        if v >= 2:
            for t in range(fine_cols // LANES):
                spot = pl.ds(LANES * t, LANES)
                edge_low[v - 2, :, spot] = held[v, t, pl.ds(0, fine_rows), :]
                edge_high[v - 2, :, spot] = held[v, t, pl.ds((levels - 1) * fine_rows, fine_rows), :]
        means = exact_dot(sums[pl.ds(v * rows * levels, rows * levels), :], table)
        slabs = [means[r * levels : (r + 1) * levels] for r in range(rows)]
        for r in range(rows):
            coarse[v, r] = slabs[r]
        for out, seq in ((up, slabs[:H_ST]), (down, slabs[rows - H_ST :])):
            for i, value in enumerate(pack_quad(seq, cols)):
                out[v, i] = value


def fill_slots(out, base, slabs, h, group_source, cols):
    per = slots_of(h)
    acc = None
    for index, item in enumerate(slabs):
        group, slot = divmod(index, per)
        value = group_source.slab(*item, slice(None))
        acc = put_slot(jnp.zeros_like(value) if slot == 0 else acc, value, slot, h, cols)
        if slot == per - 1 or index == len(slabs) - 1:
            out[base + group] = acc


def early_groups(rows):
    inc, mis = early_slabs(rows)
    count_inc = ceil_div(len(inc), slots_of(H_INC))
    return count_inc, count_inc + ceil_div(len(mis), slots_of(H_MIS))


def pack_x_early_kernel(inc, mis, top, bottom, edge_x, out, *, rows, cols):
    source = Early(inc, mis, top, bottom, rows, cols, *ends("gy"))
    slabs_inc, slabs_mis = early_slabs(rows)
    count_inc, count = early_groups(rows)
    fill_slots(out, 0, slabs_inc, H_INC, source, cols)
    fill_slots(out, count_inc, slabs_mis, H_MIS, source, cols)
    for g in range(edge_x.shape[0]):
        out[count + g] = edge_x[g]


def pack_x_late_kernel(coarse, top, bottom, out, *, rows, cols):
    source = Late(coarse, top, bottom, rows, cols, *ends("gy"))
    fill_slots(out, 0, late_slabs(rows, coarse.shape[0]), H_ST, source, cols)


def joined_early(source, pl_ref, pr_ref, rows, cols, lev):
    slabs_inc, slabs_mis = early_slabs(rows)
    count_inc, _ = early_groups(rows)
    for base, slabs, h in ((0, slabs_inc, H_INC), (count_inc, slabs_mis, H_MIS)):
        for index, item in enumerate(slabs):
            group, slot = divmod(index, slots_of(h))
            own = source.slab(*item, lev)
            value = join_columns(
                own, pl_ref[base + group, lev, :], pr_ref[base + group, lev, :], slot, h, cols
            )
            yield item, value


def joined_late(source, pl_ref, pr_ref, rows, cols, lev, count):
    for index, item in enumerate(late_slabs(rows, count)):
        group, slot = divmod(index, slots_of(H_ST))
        own = source.slab(*item, lev)
        value = join_columns(own, pl_ref[group, lev, :], pr_ref[group, lev, :], slot, H_ST, cols)
        yield item, value


def near_tile(levels):
    return pl.ds(pl.multiple_of((1 - lax.axis_index("lev")) * (levels - TILE), TILE), TILE)


def pack_l_early_kernel(inc, mis, top, bottom, px_l, px_r, low, high, out, out_edge, *, levels, rows, cols):
    source = Early(inc, mis, top, bottom, rows, cols, *ends("gy"))
    lev = near_tile(levels)
    for index, (_, value) in enumerate(joined_early(source, px_l, px_r, rows, cols, lev)):
        out[index] = value
    lower = lax.axis_index("lev") == 0
    for v in range(3):
        out_edge[v] = jnp.where(lower, high[v], low[v])


def pack_l_late_kernel(coarse, top, bottom, px_l, px_r, out, *, levels, rows, cols):
    source = Late(coarse, top, bottom, rows, cols, *ends("gy"))
    lev = near_tile(levels)
    items = joined_late(source, px_l, px_r, rows, cols, lev, coarse.shape[0])
    for index, (_, value) in enumerate(items):
        out[index] = value


def slope(p):
    squashed = jnp.tanh(p)
    return damping * (1.0 - squashed * squashed)


def chain_kernel(
    state, wind, inc, mis, top_e, bottom_e, xe_l, xe_r, le, coarse, top_t, bottom_t, xt_l, xt_r, lt,
    edge_top, edge_bottom, edge_lev, new, gradient,
    held, result, w_inc, w_mis, w_st, one, res, adj, s_c, s_t, upd, wide, fnew, fside, flev, sems, out_sems,
    *, levels, rows, cols,
):
    fine_rows = ratio * rows
    fine_cols = ratio * cols
    tiles = fine_cols // LANES
    window = levels + TILE
    copies = fetch(state, wind, held, sems)
    first, last = ends("gy")
    lev_index = lax.axis_index("lev")
    own = pl.ds(pl.multiple_of(lev_index * TILE, TILE), levels)
    far = pl.ds(pl.multiple_of((1 - lev_index) * levels, TILE), TILE)

    early = Early(inc, mis, top_e, bottom_e, rows, cols, first, last)
    late = Late(coarse, top_t, bottom_t, rows, cols, first, last)
    every = slice(None)
    for index, (item, value) in enumerate(joined_early(early, xe_l, xe_r, rows, cols, every)):
        kind, v, r = item
        ref, h = (w_inc, H_INC) if kind == "inc" else (w_mis, H_MIS)
        ref[v, r + h, own, :] = value
        ref[v, r + h, far, :] = le[index]
    for index, (item, value) in enumerate(joined_late(late, xt_l, xt_r, rows, cols, every, 5)):
        _, v, r = item
        w_st[v, r + H_ST, own, :] = value
        w_st[v, r + H_ST, far, :] = lt[index]

    level = lax.broadcasted_iota(jnp.int32, (window, LANES), 0)

    def level_sum(q):
        above = jnp.where(level == window - 1, 0.0, roll(q, -1, 0))
        below = jnp.where(level == 0, 0.0, roll(q, 1, 0))
        return above + below

    def inside(r, value):
        if r < 0:
            return jnp.where(first, 0.0, value)
        if r >= rows:
            return jnp.where(last, 0.0, value)
        return value

    half = 0.5 * advect

    def forward(ref, v, h, r):
        k = mixing[v]
        q, up, down = ref[v, r + h], ref[v, r + h - 1], ref[v, r + h + 1]
        right, left = roll(q, -1, 1), roll(q, 1, 1)
        wu, wv = w_st[0, r + H_ST], w_st[1, r + H_ST]
        spread = k * ((right + left) + (down + up)) + vertical_mix * level_sum(q)
        drift = (half * wu) * (right - left) + (half * wv) * (down - up)
        return (1.0 - 4.0 * k - 2.0 * vertical_mix) * q + (spread - drift)

    def adjoint(ref, v, h, r):
        k = mixing[v]
        q, up, down = ref[v, r + h], ref[v, r + h - 1], ref[v, r + h + 1]
        wu = half * w_st[0, r + H_ST]
        wv_up, wv_down = half * w_st[1, r + H_ST - 1], half * w_st[1, r + H_ST + 1]
        flux, kq = wu * q, k * q
        along_x = roll(kq + flux, -1, 1) + roll(kq - flux, 1, 1)
        along_y = (k + wv_down) * down + (k - wv_up) * up
        return (1.0 - 4.0 * k - 2.0 * vertical_mix) * q + ((along_x + along_y) + vertical_mix * level_sum(q))

    for v in range(3):
        for r in range(-H_ST, rows + H_ST):
            t = jnp.tanh(w_st[2 + v, r + H_ST])
            s = damping * (1.0 - t * t)
            if -2 < r < rows + 1:
                s_c[v, r + 1] = s
            value = forward(w_inc, v, H_INC, r) - s * w_inc[v, r + H_INC]
            one[v, r + H_ST] = inside(r, value)
            if -H_ST < r < rows + H_ST - 1:
                path = forward_state(w_st, v, r, forward) - damping * t
                if -H_MIS <= r < rows + H_MIS:
                    s_t[v, r + H_MIS] = slope(path)
        for r in range(-H_MIS, rows + H_MIS):
            value = forward(one, v, H_ST, r) - s_t[v, r + H_MIS] * one[v, r + H_ST]
            res[v, r + H_MIS] = inside(r, value - w_mis[v, r + H_MIS])
        for r in range(-2, rows + 2):
            value = adjoint(res, v, H_MIS, r) - s_t[v, r + H_MIS] * res[v, r + H_MIS]
            adj[v, r + 2] = inside(r, value)
        for r in range(-1, rows + 1):
            value = adjoint(adj, v, 2, r) - s_c[v, r + 1] * adj[v, r + 2]
            base = w_inc[v, r + H_INC]
            grad = base + value
            upd[v, r + 1] = inside(r, base - descent * grad)
            if 0 <= r < rows:
                one[v, r] = grad
                gradient[v, r] = one[v, r, own, :]

    source_col = lax.broadcasted_iota(jnp.int32, (LANES, fine_cols + LANES), 0)
    place = lax.broadcasted_iota(jnp.int32, (LANES, fine_cols + LANES), 1)
    place = jnp.where(place == fine_cols + LANES - 1, -1, place)
    place = jnp.where(place > fine_cols, 2 * fine_cols, place)
    scaled = 2 * place + 5
    below = (scaled + 8) // 8 - 2
    part = ((scaled + 8) % 8).astype(f32) * 0.125
    column = jnp.where(source_col == LANES - 1, -1, source_col)
    table = jnp.where(column == below, 1.0 - part, 0.0) + jnp.where(column == below + 1, part, 0.0)
    table = table.astype(bf16)
    for v in range(3):
        flat = upd[v].reshape((rows + 2) * window, LANES)
        lane = lane_of(flat.shape)
        live = jnp.logical_or(lane <= cols, lane == LANES - 1)
        flat = jnp.where(live, flat, 0.0)
        wide[v] = exact_dot(flat, table).reshape(rows + 2, window, fine_cols + LANES)

    def weights(f):
        j, a = divmod(f, ratio)
        if a < 2:
            return j, (0.375, 0.625) if a == 0 else (0.125, 0.875)
        return j + 1, (0.875, 0.125) if a == 2 else (0.625, 0.375)

    far_level = jnp.where(lev_index == 0, levels, TILE - 1)
    lower = lev_index == 0
    per = slots_of(2)
    count = early_groups(rows)[1]
    lane = lax.broadcasted_iota(jnp.int32, (levels, LANES), 1)
    sub = lax.broadcasted_iota(jnp.int32, (levels, fine_cols), 0)

    def strided(v, f):
        return jnp.concatenate(
            [held[v, t, pl.ds(f, levels, stride=fine_rows), :] for t in range(tiles)], axis=1
        )

    for v in range(3):
        wait_all(copies[v])
    outs = []
    for v in range(3):
        if v > 0:
            wait_all(copies[2 + v])
        for f in range(-1, fine_rows + 1):
            j, (w0, w1) = weights(f)
            rise = w0 * wide[v, j, own, :] + w1 * wide[v, j + 1, own, :]
            if f < 0:
                value = jnp.where(first, 0.0, edge_top[v] + rise[:, :fine_cols])
            elif f >= fine_rows:
                value = jnp.where(last, 0.0, edge_bottom[v] + rise[:, :fine_cols])
            else:
                value = strided(2 + v, f) + rise[:, :fine_cols]
                group, slot = divmod(v * fine_rows + f, per)
                back = -(4 * slot + 2)
                left = roll(xe_l[count + group], back, 1)
                right = roll(xe_r[count + group], back, 1)
                fside[f] = jnp.where(lane < LANES // 2, right, left) + rise[:, fine_cols:]
                rise_far = w0 * wide[v, j, pl.ds(far_level, 1), :] + w1 * wide[v, j + 1, pl.ds(far_level, 1), :]
                flev[pl.ds(f, 1), :] = edge_lev[v, pl.ds(f, 1), :] + rise_far[:, :fine_cols]
            fnew[f + 1] = value
        k = mixing[v]
        for f in range(fine_rows):
            q, up, down = fnew[f + 1], fnew[f], fnew[f + 2]
            parts = [q[:, LANES * t : LANES * (t + 1)] for t in range(tiles)]
            side = fside[f]
            fwd = [roll(p, -1, 1) for p in parts + [side]]
            bwd = [roll(p, 1, 1) for p in [side] + parts]
            right = jnp.concatenate([jnp.where(lane < LANES - 1, fwd[t], fwd[t + 1]) for t in range(tiles)], axis=1)
            left = jnp.concatenate([jnp.where(lane > 0, bwd[t + 1], bwd[t]) for t in range(tiles)], axis=1)
            beyond = flev[pl.ds(f, 1), :]
            above = jnp.where(sub == levels - 1, jnp.where(lower, beyond, 0.0), roll(q, -1, 0))
            under = jnp.where(sub == 0, jnp.where(lower, 0.0, beyond), roll(q, 1, 0))
            wu, wv = strided(0, f), strided(1, f)
            spread = k * ((right + left) + (down + up)) + vertical_mix * (above + under)
            drift = (half * wu) * (right - left) + (half * wv) * (down - up)
            value = (1.0 - 4.0 * k - 2.0 * vertical_mix) * q + (spread - drift) - damping * jnp.tanh(q)
            for t in range(tiles):
                result[v, t, pl.ds(f, levels, stride=fine_rows), :] = value[:, LANES * t : LANES * (t + 1)]
        for t in range(tiles):
            spot = new.at[v, :, pl.ds(LANES * t, LANES)]
            outs.append(pltpu.make_async_copy(result.at[v, t], spot, out_sems.at[v, t]))
            outs[-1].start()
    wait_all(outs)


def forward_state(ref, v, r, forward):
    class Shifted:
        def __getitem__(self, key):
            return ref[(key[0] + 2,) + key[1:]]

    return forward(Shifted(), v, H_ST, r)


VM = pl.BlockSpec(memory_space=pltpu.VMEM)
ANY = pl.BlockSpec(memory_space=pl.ANY)


def shape(*dims):
    return jax.ShapeDtypeStruct(dims, f32)


def cost(flops):
    return pl.CostEstimate(flops=flops, bytes_accessed=flops, transcendentals=0)


def ring(axis):
    count = lax.axis_size(axis)
    ahead = [(i, (i + 1) % count) for i in range(count)]
    return ahead, [(b, a) for a, b in ahead]


def side_exchange(payload):
    ahead, back = ring("gx")
    from_left = lax.ppermute(payload, "gx", ahead)
    if lax.axis_size("gx") == 2:
        return from_left, from_left
    return from_left, lax.ppermute(payload, "gx", back)


def per_device(fine_state, wind_field, increment, misfit):
    _, levels, rows, cols = increment.shape
    fine_rows, fine_cols = fine_state.shape[2:]
    assert 4 * cols == 3 * LANES and levels % TILE == 0 and rows >= H_INC
    assert lax.axis_size("lev") == 2
    state = fine_state.reshape(3, levels * fine_rows, fine_cols)
    wind = wind_field.reshape(2, levels * fine_rows, fine_cols)
    sizes = dict(rows=rows, cols=cols)
    up_ring, down_ring = ring("gy")[1], ring("gy")[0]
    swap = [(0, 1), (1, 0)]

    def slabs(x):
        return jnp.pad(jnp.transpose(x, (0, 2, 1, 3)), ((0, 0), (0, 0), (0, 0), (0, LANES - cols)))

    inc, mis = slabs(increment), slabs(misfit)
    up_e, down_e = pl.pallas_call(
        functools.partial(pack_early_kernel, **sizes),
        out_shape=(shape(3, 2, 3, levels, LANES),) * 2,
        in_specs=[VM] * 2, out_specs=[VM] * 2, cost_estimate=cost(10**5), name="pack_early",
    )(inc, mis)
    bottom_e = lax.ppermute(up_e, "gy", up_ring)
    top_e = lax.ppermute(down_e, "gy", down_ring)

    groups_x = ceil_div(3 * fine_rows, slots_of(2))
    coarse, up_t, down_t, edge_up, edge_down, edge_x, edge_low, edge_high = pl.pallas_call(
        functools.partial(mean_kernel, levels=levels, **sizes),
        out_shape=(
            shape(5, rows, levels, LANES), shape(5, 3, levels, LANES), shape(5, 3, levels, LANES),
            shape(3, levels, fine_cols), shape(3, levels, fine_cols), shape(groups_x, levels, LANES),
            shape(3, fine_rows, fine_cols), shape(3, fine_rows, fine_cols),
        ),
        in_specs=[ANY] * 2, out_specs=[VM] * 8,
        scratch_shapes=[
            pltpu.VMEM((5, fine_cols // LANES, levels * fine_rows, LANES), f32),
            pltpu.VMEM((5 * rows * levels, fine_cols), f32),
            pltpu.SemaphoreType.DMA((5, fine_cols // LANES)),
        ],
        cost_estimate=cost(10**7), name="block_mean",
        compiler_params=pltpu.CompilerParams(vmem_limit_bytes=24 * 2**20),
    )(state, wind)
    bottom_t = lax.ppermute(up_t, "gy", up_ring)
    top_t = lax.ppermute(down_t, "gy", down_ring)
    edge_bottom = lax.ppermute(edge_up, "gy", up_ring)
    edge_top = lax.ppermute(edge_down, "gy", down_ring)

    count_e = early_groups(rows)[1]
    pay_xe = pl.pallas_call(
        functools.partial(pack_x_early_kernel, **sizes),
        out_shape=shape(count_e + groups_x, levels, LANES),
        in_specs=[VM] * 5, out_specs=VM, cost_estimate=cost(10**6), name="pack_x_early",
    )(inc, mis, top_e, bottom_e, edge_x)
    xe_l, xe_r = side_exchange(pay_xe)
    number_e = sum(len(s) for s in early_slabs(rows))
    pay_le, pay_edge = pl.pallas_call(
        functools.partial(pack_l_early_kernel, levels=levels, **sizes),
        out_shape=(shape(number_e, TILE, LANES), shape(3, fine_rows, fine_cols)),
        in_specs=[VM] * 8, out_specs=[VM] * 2, cost_estimate=cost(10**6), name="pack_l_early",
    )(inc, mis, top_e, bottom_e, xe_l, xe_r, edge_low, edge_high)
    le = lax.ppermute(pay_le, "lev", swap)
    edge_lev = lax.ppermute(pay_edge, "lev", swap)

    number_t = len(late_slabs(rows, 5))
    pay_xt = pl.pallas_call(
        functools.partial(pack_x_late_kernel, **sizes),
        out_shape=shape(ceil_div(number_t, slots_of(H_ST)), levels, LANES),
        in_specs=[VM] * 3, out_specs=VM, cost_estimate=cost(10**6), name="pack_x_late",
    )(coarse, top_t, bottom_t)
    xt_l, xt_r = side_exchange(pay_xt)
    pay_lt = pl.pallas_call(
        functools.partial(pack_l_late_kernel, levels=levels, **sizes),
        out_shape=shape(number_t, TILE, LANES),
        in_specs=[VM] * 5, out_specs=VM, cost_estimate=cost(10**6), name="pack_l_late",
    )(coarse, top_t, bottom_t, xt_l, xt_r)
    lt = lax.ppermute(pay_lt, "lev", swap)

    window = levels + TILE

    def scratch(count, extra):
        return pltpu.VMEM((count, rows + 2 * extra, window, LANES), f32)

    new, grad = pl.pallas_call(
        functools.partial(chain_kernel, levels=levels, **sizes),
        out_shape=(shape(*state.shape), shape(3, rows, levels, LANES)),
        in_specs=[ANY] * 2 + [VM] * 16, out_specs=[ANY, VM],
        scratch_shapes=[
            pltpu.VMEM((5, fine_cols // LANES, levels * fine_rows, LANES), f32),
            pltpu.VMEM((3, fine_cols // LANES, levels * fine_rows, LANES), f32),
            scratch(3, H_INC), scratch(3, H_MIS), scratch(5, H_ST),
            scratch(3, H_ST), scratch(3, H_MIS), scratch(3, 2), scratch(3, 1), scratch(3, H_MIS), scratch(3, 1),
            pltpu.VMEM((3, rows + 2, window, fine_cols + LANES), f32),
            pltpu.VMEM((fine_rows + 2, levels, fine_cols), f32),
            pltpu.VMEM((fine_rows, levels, LANES), f32),
            pltpu.VMEM((fine_rows, fine_cols), f32),
            pltpu.SemaphoreType.DMA((5, fine_cols // LANES)), pltpu.SemaphoreType.DMA((3, fine_cols // LANES)),
        ],
        cost_estimate=cost(10**7), name="chain",
        compiler_params=pltpu.CompilerParams(vmem_limit_bytes=40 * 2**20),
    )(
        state, wind, inc, mis, top_e, bottom_e, xe_l, xe_r, le, coarse, top_t, bottom_t, xt_l, xt_r, lt,
        edge_top, edge_bottom, edge_lev,
    )
    gradient = jnp.transpose(grad[..., :cols], (0, 2, 1, 3))
    return new.reshape(fine_state.shape), gradient


def solution(mesh):
    spec = P(None, "lev", "gy", "gx")
    return jax.shard_map(
        per_device, mesh=mesh, in_specs=(spec,) * 4, out_specs=(spec,) * 2, check_vma=False
    )
```

```python
import functools

import jax
import jax.numpy as jnp
from jax import lax
from jax.experimental import pallas as pl
from jax.experimental.pallas import tpu as pltpu
from jax.sharding import PartitionSpec as P


advect = 0.25
vertical_mix = 0.1
damping = 0.3
descent = 0.5
mixing = (0.05, 0.1, 0.2)
ratio = 4
LANES = 128
TILE = 8
H_INC, H_ST, H_MIS = 5, 4, 3
f32 = jnp.float32
bf16 = jnp.bfloat16


def roll(x, shift, axis):
    size = x.shape[axis]
    shift = shift % size
    return x if shift == 0 else pltpu.roll(x, shift, axis)


def lane_of(shape):
    return lax.broadcasted_iota(jnp.int32, shape, len(shape) - 1)


def split3(x):
    hi = x.astype(bf16)
    rest = x - hi.astype(f32)
    mid = rest.astype(bf16)
    low = (rest - mid.astype(f32)).astype(bf16)
    return hi, mid, low


def exact_dot(x, table):
    hi, mid, low = split3(x)
    dot = functools.partial(jnp.dot, preferred_element_type=f32)
    return dot(hi, table) + (dot(mid, table) + dot(low, table))


def pack_quad(rows, cols):
    r0, r1, r2, r3 = rows
    lane = lane_of(r0.shape)
    t1 = roll(r1, cols, 1)
    t2 = roll(r2, 2 * cols - LANES, 1)
    t3 = roll(r3, 3 * cols - 2 * LANES, 1)
    return (
        jnp.where(lane < cols, r0, t1),
        jnp.where(lane < 2 * cols - LANES, t1, t2),
        jnp.where(lane < 3 * cols - 2 * LANES, t2, t3),
    )


def unpack_quad(packed, index, cols):
    p0, p1, p2 = packed
    if index == 0:
        return p0
    lane = lane_of(p0.shape)
    if index == 1:
        edge = LANES - cols
        return jnp.where(lane < edge, roll(p0, edge, 1), roll(p1, edge, 1))
    if index == 2:
        edge = 2 * (LANES - cols)
        return jnp.where(lane < edge, roll(p1, edge, 1), roll(p2, edge, 1))
    return roll(p2, 3 * (LANES - cols), 1)


def slots_of(h):
    return LANES // (2 * h)


def fill_slots(slabs, h, cols):
    lane = lane_of(slabs[0].shape)
    outer = jnp.logical_or(lane < h, jnp.logical_and(lane >= cols - h, lane < cols))
    kept = [jnp.where(outer, x, 0.0) for x in slabs]
    moved = [roll(x, 2 * h * i, 1) for i, x in enumerate(kept)]
    while len(moved) > 1:
        moved = [sum(moved[i : i + 2]) for i in range(0, len(moved), 2)]
    return moved[0]


def join_columns(owns, from_left, from_right, h, cols):
    lane = lane_of(owns[0].shape)
    lefts = [roll(from_left, LANES - cols - 2 * h * i, 1) for i in range(len(owns))]
    rights = [roll(from_right, cols - 2 * h * i, 1) for i in range(len(owns))]
    middle = (cols + LANES) // 2
    return [
        jnp.where(lane < cols, own, jnp.where(lane < middle, right, left))
        for own, left, right in zip(owns, lefts, rights)
    ]


def ceil_div(a, b):
    return -(-a // b)


S_INC, S_ST = 8, 4


def early_slabs(rows):
    inc = [("inc", v, r) for v in range(3) for r in range(-H_INC, rows + H_INC)]
    mis = [("mis", v, r) for v in range(3) for r in range(-H_MIS, rows + H_MIS)]
    return inc + mis


def late_slabs(rows, count):
    return [("st", v, r) for v in range(count) for r in range(-H_ST, rows + H_ST)]


def batches(slabs):
    found, start = [], 0
    while start < len(slabs):
        kind = slabs[start][0]
        h = S_INC if kind == "inc" else S_ST
        stop = start
        while stop < len(slabs) and stop - start < slots_of(h) and slabs[stop][0] == kind:
            stop += 1
        found.append((start, stop - start, h))
        start = stop
    return found


def unpack(top, bottom, place, cols):
    return [
        [unpack_quad(tuple(ref[place + (i,)] for i in range(3)), index, cols) for index in range(4)]
        for ref in (top, bottom)
    ]


def ends(axis):
    place = lax.axis_index(axis)
    return place == 0, place == lax.axis_size(axis) - 1


def fetch(state, wind, held, sems):
    copies = []
    for v in range(5):
        source = wind.at[v] if v < 2 else state.at[v - 2]
        copies.append([])
        for t in range(held.shape[1]):
            part = source.at[:, pl.ds(LANES * t, LANES)]
            copies[-1].append(pltpu.make_async_copy(part, held.at[v, t], sems.at[v, t]))
            copies[-1][-1].start()
    return copies


def wait_all(copies):
    for c in copies:
        c.wait()


def pack_early_kernel(increment, misfit, inc, mis, up, down, *, rows, cols):
    levels = increment.shape[1]
    for v in range(3):
        for source, out in ((increment, inc), (misfit, mis)):
            turned = jnp.transpose(source[v], (1, 0, 2))
            blank = jnp.zeros((levels, LANES - cols), f32)
            for r in range(rows):
                out[v, r] = jnp.concatenate([turned[r], blank], axis=1)
    for v in range(3):
        first = [inc[v, r] for r in range(H_INC)] + [mis[v, r] for r in range(H_MIS)]
        last = [inc[v, rows - H_INC + r] for r in range(H_INC)]
        last += [mis[v, rows - H_MIS + r] for r in range(H_MIS)]
        for out, seq in ((up, first), (down, last)):
            for quad in range(2):
                for i, value in enumerate(pack_quad(seq[4 * quad : 4 * quad + 4], cols)):
                    out[v, quad, i] = value


def mean_kernel(
    state, wind, coarse, up, down, edge_up, edge_down, edge_x, edge_low, edge_high,
    held, sums, sems, *, levels, rows, cols,
):
    fine_rows = ratio * rows
    fine_cols = ratio * cols
    copies = fetch(state, wind, held, sems)
    source_col = lax.broadcasted_iota(jnp.int32, (fine_cols, LANES), 0)
    target_col = lax.broadcasted_iota(jnp.int32, (fine_cols, LANES), 1)
    table = jnp.where(source_col // ratio == target_col, 1.0 / (ratio * ratio), 0.0).astype(bf16)
    slot_h = 2
    per = slots_of(slot_h)
    acc = None
    for v in range(5):
        wait_all(copies[v])
        for row in range(rows):
            total = None
            for a in range(ratio):
                f = ratio * row + a
                pieces = [
                    held[v, t, pl.ds(f, levels, stride=fine_rows), :]
                    for t in range(fine_cols // LANES)
                ]
                slab = jnp.concatenate(pieces, axis=1)
                total = slab if total is None else total + slab
                if v >= 2:
                    if f == 0:
                        edge_up[v - 2] = slab
                    if f == fine_rows - 1:
                        edge_down[v - 2] = slab
                    index = (v - 2) * fine_rows + f
                    group, slot = divmod(index, per)
                    lane = lane_of(pieces[0].shape)
                    seam = jnp.where(lane < LANES // 2, pieces[0], pieces[-1])
                    moved = roll(seam, 2 * slot_h * slot + slot_h, 1)
                    if slot == 0:
                        acc = moved
                    else:
                        acc = jnp.where(lane >= 2 * slot_h * slot, moved, acc)
                    if slot == per - 1 or index == 3 * fine_rows - 1:
                        edge_x[group] = acc
            sums[pl.ds((v * rows + row) * levels, levels), :] = total
        if v >= 2:
            for t in range(fine_cols // LANES):
                spot = pl.ds(LANES * t, LANES)
                edge_low[v - 2, :, spot] = held[v, t, pl.ds(0, fine_rows), :]
                edge_high[v - 2, :, spot] = held[v, t, pl.ds((levels - 1) * fine_rows, fine_rows), :]
        means = exact_dot(sums[pl.ds(v * rows * levels, rows * levels), :], table)
        slabs = [means[r * levels : (r + 1) * levels] for r in range(rows)]
        for r in range(rows):
            coarse[v, r] = slabs[r]
        for out, seq in ((up, slabs[:H_ST]), (down, slabs[rows - H_ST :])):
            for i, value in enumerate(pack_quad(seq, cols)):
                out[v, i] = value


def pack_x(rows_ref, slabs, out, cols):
    for group, (start, number, h) in enumerate(batches(slabs)):
        out[group] = fill_slots([rows_ref[start + i] for i in range(number)], h, cols)


def pack_x_early_kernel(inc, mis, top, bottom, edge_x, ext, out, *, rows, cols):
    first, last = ends("gy")
    slabs = early_slabs(rows)
    index = {item: i for i, item in enumerate(slabs)}
    for v in range(3):
        for r in range(rows):
            ext[index["inc", v, r]] = inc[v, r]
            ext[index["mis", v, r]] = mis[v, r]
        above, below = [], []
        for quad in range(2):
            one, two = unpack(top, bottom, (v, quad), cols)
            above += one
            below += two
        for p in range(H_INC + H_MIS):
            kind, h, q = ("inc", H_INC, p) if p < H_INC else ("mis", H_MIS, p - H_INC)
            ext[index[kind, v, q - h]] = jnp.where(first, 0.0, above[p])
            ext[index[kind, v, rows + q]] = jnp.where(last, 0.0, below[p])
    pack_x(ext, slabs, out, cols)
    count = len(batches(slabs))
    for g in range(edge_x.shape[0]):
        out[count + g] = edge_x[g]


def pack_x_late_kernel(coarse, top, bottom, ext, out, *, rows, cols):
    first, last = ends("gy")
    count = coarse.shape[0]
    slabs = late_slabs(rows, count)
    index = {item: i for i, item in enumerate(slabs)}
    for v in range(count):
        for r in range(rows):
            ext[index["st", v, r]] = coarse[v, r]
        above, below = unpack(top, bottom, (v,), cols)
        for p in range(H_ST):
            ext[index["st", v, p - H_ST]] = jnp.where(first, 0.0, above[p])
            ext[index["st", v, rows + p]] = jnp.where(last, 0.0, below[p])
    pack_x(ext, slabs, out, cols)


def join_all(ext, from_left, from_right, slabs, out, lev, cols):
    for group, (start, number, h) in enumerate(batches(slabs)):
        owns = [ext[start + i, lev, :] for i in range(number)]
        joined = join_columns(owns, from_left[group, lev, :], from_right[group, lev, :], h, cols)
        for i, value in enumerate(joined):
            out[start + i] = value


def near_tile(levels):
    return pl.ds(pl.multiple_of((1 - lax.axis_index("lev")) * (levels - TILE), TILE), TILE)


def pack_l_kernel(ext, from_left, from_right, out, *, levels, slabs, cols):
    join_all(ext, from_left, from_right, slabs, out, near_tile(levels), cols)


def join_kernel(ext, from_left, from_right, out, *, slabs, cols):
    join_all(ext, from_left, from_right, slabs, out, slice(None), cols)


def slope(p):
    squashed = jnp.tanh(p)
    return damping * (1.0 - squashed * squashed)


def chain_kernel(
    state, wind, own_e, xe_l, xe_r, le, own_t, lt, edge_top, edge_bottom, edge_lev, new, gradient,
    held, result, w_inc, w_mis, w_st, one, res, adj, s_c, s_t, upd, wide, fnew, fside, flev, sems, out_sems,
    *, levels, rows, cols,
):
    fine_rows = ratio * rows
    fine_cols = ratio * cols
    tiles = fine_cols // LANES
    window = levels + TILE
    copies = fetch(state, wind, held, sems)
    first, last = ends("gy")
    lev_index = lax.axis_index("lev")
    own = pl.ds(pl.multiple_of(lev_index * TILE, TILE), levels)
    far = pl.ds(pl.multiple_of((1 - lev_index) * levels, TILE), TILE)

    for index, (kind, v, r) in enumerate(early_slabs(rows)):
        ref, h = (w_inc, H_INC) if kind == "inc" else (w_mis, H_MIS)
        ref[v, r + h, own, :] = own_e[index]
        ref[v, r + h, far, :] = le[index]
    for index, (_, v, r) in enumerate(late_slabs(rows, 5)):
        w_st[v, r + H_ST, own, :] = own_t[index]
        w_st[v, r + H_ST, far, :] = lt[index]

    level = lax.broadcasted_iota(jnp.int32, (window, LANES), 0)

    def level_sum(q):
        above = jnp.where(level == window - 1, 0.0, roll(q, -1, 0))
        below = jnp.where(level == 0, 0.0, roll(q, 1, 0))
        return above + below

    def inside(r, value):
        if r < 0:
            return jnp.where(first, 0.0, value)
        if r >= rows:
            return jnp.where(last, 0.0, value)
        return value

    half = 0.5 * advect

    def forward(ref, v, h, r):
        k = mixing[v]
        q, up, down = ref[v, r + h], ref[v, r + h - 1], ref[v, r + h + 1]
        right, left = roll(q, -1, 1), roll(q, 1, 1)
        wu, wv = w_st[0, r + H_ST], w_st[1, r + H_ST]
        spread = k * ((right + left) + (down + up)) + vertical_mix * level_sum(q)
        drift = (half * wu) * (right - left) + (half * wv) * (down - up)
        return (1.0 - 4.0 * k - 2.0 * vertical_mix) * q + (spread - drift)

    def adjoint(ref, v, h, r):
        k = mixing[v]
        q, up, down = ref[v, r + h], ref[v, r + h - 1], ref[v, r + h + 1]
        wu = half * w_st[0, r + H_ST]
        wv_up, wv_down = half * w_st[1, r + H_ST - 1], half * w_st[1, r + H_ST + 1]
        flux, kq = wu * q, k * q
        along_x = roll(kq + flux, -1, 1) + roll(kq - flux, 1, 1)
        along_y = (k + wv_down) * down + (k - wv_up) * up
        return (1.0 - 4.0 * k - 2.0 * vertical_mix) * q + ((along_x + along_y) + vertical_mix * level_sum(q))

    for v in range(3):
        for r in range(-H_ST, rows + H_ST):
            t = jnp.tanh(w_st[2 + v, r + H_ST])
            s = damping * (1.0 - t * t)
            if -2 < r < rows + 1:
                s_c[v, r + 1] = s
            value = forward(w_inc, v, H_INC, r) - s * w_inc[v, r + H_INC]
            one[v, r + H_ST] = inside(r, value)
            if -H_ST < r < rows + H_ST - 1:
                path = forward_state(w_st, v, r, forward) - damping * t
                if -H_MIS <= r < rows + H_MIS:
                    s_t[v, r + H_MIS] = slope(path)
        for r in range(-H_MIS, rows + H_MIS):
            value = forward(one, v, H_ST, r) - s_t[v, r + H_MIS] * one[v, r + H_ST]
            res[v, r + H_MIS] = inside(r, value - w_mis[v, r + H_MIS])
        for r in range(-2, rows + 2):
            value = adjoint(res, v, H_MIS, r) - s_t[v, r + H_MIS] * res[v, r + H_MIS]
            adj[v, r + 2] = inside(r, value)
        for r in range(-1, rows + 1):
            value = adjoint(adj, v, 2, r) - s_c[v, r + 1] * adj[v, r + 2]
            base = w_inc[v, r + H_INC]
            grad = base + value
            upd[v, r + 1] = inside(r, base - descent * grad)
            if 0 <= r < rows:
                one[v, r] = grad
        turned = jnp.stack([one[v, r, own, :] for r in range(rows)])
        gradient[v] = jnp.transpose(turned, (1, 0, 2))[:, :, :cols]

    source_col = lax.broadcasted_iota(jnp.int32, (LANES, fine_cols + LANES), 0)
    place = lax.broadcasted_iota(jnp.int32, (LANES, fine_cols + LANES), 1)
    place = jnp.where(place == fine_cols + LANES - 1, -1, place)
    place = jnp.where(place > fine_cols, 2 * fine_cols, place)
    scaled = 2 * place + 5
    below = (scaled + 8) // 8 - 2
    part = ((scaled + 8) % 8).astype(f32) * 0.125
    column = jnp.where(source_col == LANES - 1, -1, source_col)
    table = jnp.where(column == below, 1.0 - part, 0.0) + jnp.where(column == below + 1, part, 0.0)
    table = table.astype(bf16)
    for v in range(3):
        flat = upd[v].reshape((rows + 2) * window, LANES)
        lane = lane_of(flat.shape)
        live = jnp.logical_or(lane <= cols, lane == LANES - 1)
        flat = jnp.where(live, flat, 0.0)
        wide[v] = exact_dot(flat, table).reshape(rows + 2, window, fine_cols + LANES)

    def weights(f):
        j, a = divmod(f, ratio)
        if a < 2:
            return j, (0.375, 0.625) if a == 0 else (0.125, 0.875)
        return j + 1, (0.875, 0.125) if a == 2 else (0.625, 0.375)

    far_level = jnp.where(lev_index == 0, levels, TILE - 1)
    lower = lev_index == 0
    per = slots_of(2)
    count = len(batches(early_slabs(rows)))
    lane = lax.broadcasted_iota(jnp.int32, (levels, LANES), 1)
    sub = lax.broadcasted_iota(jnp.int32, (levels, fine_cols), 0)

    def strided(v, f):
        return jnp.concatenate(
            [held[v, t, pl.ds(f, levels, stride=fine_rows), :] for t in range(tiles)], axis=1
        )

    for v in range(3):
        wait_all(copies[v])
    outs = []
    for v in range(3):
        if v > 0:
            wait_all(copies[2 + v])
        for f in range(-1, fine_rows + 1):
            j, (w0, w1) = weights(f)
            rise = w0 * wide[v, j, own, :] + w1 * wide[v, j + 1, own, :]
            if f < 0:
                value = jnp.where(first, 0.0, edge_top[v] + rise[:, :fine_cols])
            elif f >= fine_rows:
                value = jnp.where(last, 0.0, edge_bottom[v] + rise[:, :fine_cols])
            else:
                value = strided(2 + v, f) + rise[:, :fine_cols]
                group, slot = divmod(v * fine_rows + f, per)
                back = -(4 * slot + 2)
                left = roll(xe_l[count + group], back, 1)
                right = roll(xe_r[count + group], back, 1)
                fside[f] = jnp.where(lane < LANES // 2, right, left) + rise[:, fine_cols:]
                rise_far = w0 * wide[v, j, pl.ds(far_level, 1), :] + w1 * wide[v, j + 1, pl.ds(far_level, 1), :]
                flev[pl.ds(f, 1), :] = edge_lev[v, pl.ds(f, 1), :] + rise_far[:, :fine_cols]
            fnew[f + 1] = value
        k = mixing[v]
        for f in range(fine_rows):
            q, up, down = fnew[f + 1], fnew[f], fnew[f + 2]
            parts = [q[:, LANES * t : LANES * (t + 1)] for t in range(tiles)]
            side = fside[f]
            fwd = [roll(p, -1, 1) for p in parts + [side]]
            bwd = [roll(p, 1, 1) for p in [side] + parts]
            right = jnp.concatenate([jnp.where(lane < LANES - 1, fwd[t], fwd[t + 1]) for t in range(tiles)], axis=1)
            left = jnp.concatenate([jnp.where(lane > 0, bwd[t + 1], bwd[t]) for t in range(tiles)], axis=1)
            beyond = flev[pl.ds(f, 1), :]
            above = jnp.where(sub == levels - 1, jnp.where(lower, beyond, 0.0), roll(q, -1, 0))
            under = jnp.where(sub == 0, jnp.where(lower, 0.0, beyond), roll(q, 1, 0))
            wu, wv = strided(0, f), strided(1, f)
            spread = k * ((right + left) + (down + up)) + vertical_mix * (above + under)
            drift = (half * wu) * (right - left) + (half * wv) * (down - up)
            value = (1.0 - 4.0 * k - 2.0 * vertical_mix) * q + (spread - drift) - damping * jnp.tanh(q)
            for t in range(tiles):
                result[v, t, pl.ds(f, levels, stride=fine_rows), :] = value[:, LANES * t : LANES * (t + 1)]
        for t in range(tiles):
            spot = new.at[v, :, pl.ds(LANES * t, LANES)]
            outs.append(pltpu.make_async_copy(result.at[v, t], spot, out_sems.at[v, t]))
            outs[-1].start()
    wait_all(outs)


def forward_state(ref, v, r, forward):
    class Shifted:
        def __getitem__(self, key):
            return ref[(key[0] + 2,) + key[1:]]

    return forward(Shifted(), v, H_ST, r)


VM = pl.BlockSpec(memory_space=pltpu.VMEM)
ANY = pl.BlockSpec(memory_space=pl.ANY)


def shape(*dims):
    return jax.ShapeDtypeStruct(dims, f32)


def cost(flops):
    return pl.CostEstimate(flops=flops, bytes_accessed=flops, transcendentals=0)


def ring(axis):
    count = lax.axis_size(axis)
    ahead = [(i, (i + 1) % count) for i in range(count)]
    return ahead, [(b, a) for a, b in ahead]


def side_exchange(payload):
    ahead, back = ring("gx")
    from_left = lax.ppermute(payload, "gx", ahead)
    if lax.axis_size("gx") == 2:
        return from_left, from_left
    return from_left, lax.ppermute(payload, "gx", back)


def per_device(fine_state, wind_field, increment, misfit):
    _, levels, rows, cols = increment.shape
    fine_rows, fine_cols = fine_state.shape[2:]
    assert 4 * cols == 3 * LANES and levels % TILE == 0 and rows >= H_INC
    assert lax.axis_size("lev") == 2
    state = fine_state.reshape(3, levels * fine_rows, fine_cols)
    wind = wind_field.reshape(2, levels * fine_rows, fine_cols)
    sizes = dict(rows=rows, cols=cols)
    up_ring, down_ring = ring("gy")[1], ring("gy")[0]
    swap = [(0, 1), (1, 0)]

    small = pltpu.CompilerParams(vmem_limit_bytes=8 * 2**20)
    groups_x = ceil_div(3 * fine_rows, slots_of(2))
    e_slabs, t_slabs = early_slabs(rows), late_slabs(rows, 5)
    e_groups, t_groups = len(batches(e_slabs)), len(batches(t_slabs))

    inc, mis, up_e, down_e = pl.pallas_call(
        functools.partial(pack_early_kernel, **sizes),
        out_shape=(shape(3, rows, levels, LANES),) * 2 + (shape(3, 2, 3, levels, LANES),) * 2,
        in_specs=[VM] * 2, out_specs=[VM] * 4, cost_estimate=cost(10**5), name="pack_early", compiler_params=small,
    )(increment, misfit)
    bottom_e = lax.ppermute(up_e, "gy", up_ring)
    top_e = lax.ppermute(down_e, "gy", down_ring)

    coarse, up_t, down_t, edge_up, edge_down, edge_x, edge_low, edge_high = pl.pallas_call(
        functools.partial(mean_kernel, levels=levels, **sizes),
        out_shape=(
            shape(5, rows, levels, LANES), shape(5, 3, levels, LANES), shape(5, 3, levels, LANES),
            shape(3, levels, fine_cols), shape(3, levels, fine_cols), shape(groups_x, levels, LANES),
            shape(3, fine_rows, fine_cols), shape(3, fine_rows, fine_cols),
        ),
        in_specs=[ANY] * 2, out_specs=[VM] * 8,
        scratch_shapes=[
            pltpu.VMEM((5, fine_cols // LANES, levels * fine_rows, LANES), f32),
            pltpu.VMEM((5 * rows * levels, fine_cols), f32),
            pltpu.SemaphoreType.DMA((5, fine_cols // LANES)),
        ],
        cost_estimate=cost(10**7), name="block_mean",
        compiler_params=pltpu.CompilerParams(vmem_limit_bytes=12 * 2**20),
    )(state, wind)
    bottom_t = lax.ppermute(up_t, "gy", up_ring)
    top_t = lax.ppermute(down_t, "gy", down_ring)
    edge_bottom = lax.ppermute(edge_up, "gy", up_ring)
    edge_top = lax.ppermute(edge_down, "gy", down_ring)
    pay_edge = jnp.where(lax.axis_index("lev") == 0, edge_high, edge_low)
    edge_lev = lax.ppermute(pay_edge, "lev", swap)

    ext_e, pay_xe = pl.pallas_call(
        functools.partial(pack_x_early_kernel, **sizes),
        out_shape=(shape(len(e_slabs), levels, LANES), shape(e_groups + groups_x, levels, LANES)),
        in_specs=[VM] * 5, out_specs=[VM] * 2, cost_estimate=cost(10**6), name="pack_x_early", compiler_params=small,
    )(inc, mis, top_e, bottom_e, edge_x)
    xe_l, xe_r = side_exchange(pay_xe)

    def pack_l(ext, left, right, slabs):
        return pl.pallas_call(
            functools.partial(pack_l_kernel, levels=levels, slabs=slabs, cols=cols),
            out_shape=shape(len(slabs), TILE, LANES),
            in_specs=[VM] * 3, out_specs=VM, cost_estimate=cost(10**6), compiler_params=small,
        )(ext, left, right)

    def join(ext, left, right, slabs):
        return pl.pallas_call(
            functools.partial(join_kernel, slabs=slabs, cols=cols),
            out_shape=shape(len(slabs), levels, LANES),
            in_specs=[VM] * 3, out_specs=VM, cost_estimate=cost(10**6), compiler_params=small,
        )(ext, left, right)

    pay_le = pack_l(ext_e, xe_l, xe_r, e_slabs)
    le = lax.ppermute(pay_le, "lev", swap)
    own_e = join(ext_e, xe_l, xe_r, e_slabs)

    ext_t, pay_xt = pl.pallas_call(
        functools.partial(pack_x_late_kernel, **sizes),
        out_shape=(shape(len(t_slabs), levels, LANES), shape(t_groups, levels, LANES)),
        in_specs=[VM] * 3, out_specs=[VM] * 2, cost_estimate=cost(10**6), name="pack_x_late", compiler_params=small,
    )(coarse, top_t, bottom_t)
    xt_l, xt_r = side_exchange(pay_xt)
    pay_lt = pack_l(ext_t, xt_l, xt_r, t_slabs)
    lt = lax.ppermute(pay_lt, "lev", swap)
    own_t = join(ext_t, xt_l, xt_r, t_slabs)

    window = levels + TILE

    def scratch(count, extra):
        return pltpu.VMEM((count, rows + 2 * extra, window, LANES), f32)

    new, gradient = pl.pallas_call(
        functools.partial(chain_kernel, levels=levels, **sizes),
        out_shape=(shape(*state.shape), shape(*increment.shape)),
        in_specs=[ANY] * 2 + [VM] * 9, out_specs=[ANY, VM],
        scratch_shapes=[
            pltpu.VMEM((5, fine_cols // LANES, levels * fine_rows, LANES), f32),
            pltpu.VMEM((3, fine_cols // LANES, levels * fine_rows, LANES), f32),
            scratch(3, H_INC), scratch(3, H_MIS), scratch(5, H_ST),
            scratch(3, H_ST), scratch(3, H_MIS), scratch(3, 2), scratch(3, 1), scratch(3, H_MIS), scratch(3, 1),
            pltpu.VMEM((3, rows + 2, window, fine_cols + LANES), f32),
            pltpu.VMEM((fine_rows + 2, levels, fine_cols), f32),
            pltpu.VMEM((fine_rows, levels, LANES), f32),
            pltpu.VMEM((fine_rows, fine_cols), f32),
            pltpu.SemaphoreType.DMA((5, fine_cols // LANES)), pltpu.SemaphoreType.DMA((3, fine_cols // LANES)),
        ],
        cost_estimate=cost(10**7), name="chain",
        compiler_params=pltpu.CompilerParams(vmem_limit_bytes=24 * 2**20),
    )(state, wind, own_e, xe_l, xe_r, le, own_t, lt, edge_top, edge_bottom, edge_lev)
    return new.reshape(fine_state.shape), gradient


def solution(mesh):
    spec = P(None, "lev", "gy", "gx")

    return jax.shard_map(per_device, mesh=mesh, in_specs=(spec,) * 4, out_specs=(spec,) * 2, check_vma=False)
```
